32 devices in a mesh: seq: 8 (over z, x), head: 2 (over y), dp: 2 (over core).
Axes of the slice: x: 2, y: 2, z: 4, core: 2. Of those that a mesh axis runs over, the one named last changes fastest.
Arguments:
- queries: bfloat16 [8192, 4096], P(('dp', 'seq'), 'head'), parts along dimension 0, may hold values from -200 to 200
- keys: bfloat16 [8192, 1024], P(('dp', 'seq'), 'head'), parts along dimension 0, may hold values from -4 to 4
- values: bfloat16 [8192, 1024], P(('dp', 'seq'), 'head'), parts along dimension 0, may hold values from -15 to 15
- doc_ids: int32 [8192], P(('dp', 'seq')), parts along dimension 0, may hold values from 0 to 7, as said below
- block_lists: int32 [64, 16], P(('dp', 'seq')), parts along dimension 0, may hold values from 0 to 32, as said below
- w_out: bfloat16 [4096, 4096], P('head'), may hold values from -0.09375 to 0.09375
Outputs:
- mixed: bfloat16 [8192, 4096], P(('dp', 'seq'), 'head'), parts along dimension 0
The draws below stay inside these ranges and needn't reach their ends.
There are 2 independent parts, one for each index of `dp`. The reference program is written for one: setup_inputs(seed, part) draws one part's arguments, and reference() takes and returns one part's arrays. A program takes and returns all parts, laid end to end along the dimension named above; an argument that names none is the same for every part. Nothing has to cross between parts.
Inputs may be any that keep to these rules, and one draw needn't show every extreme that they name: `block_lists`: row i lists the blocks that query block i reads: 16 entries, each a block of the sequence or the null value 32; the non-null entries of a row are distinct and include i. Blocks k * 4 to k * 4 + 3 lie on index k of seq; over the rows of one index of seq together, at most one distinct block of each other index of seq is named (so each index of seq sends at most one of its blocks to each other index). `doc_ids`: never falling along the sequence.
All inputs are finite; a program needn't handle non-finite values.
Results may differ from the reference program's by a relative error of at most 0.013.
Values may be sent and summed in bfloat16 or wider, within the bound.
A program may use at most 128 MiB of HBM per device.

```python
import math
import jax
import jax.numpy as jnp
from jax import lax

D = 4096
QUERY_HEADS = 32
KEY_VALUE_HEADS = 8
HEAD_SIZE = 128
BLOCK_TOKENS = 128
TOPK = 16
DOCS = 8
SEQUENCE_TOKENS = 4096
BPD = 4
BLOCK_TOTAL = 32
N_HEAD = 2


def draw_queries(key, part):
    base_index = 2.0 * jax.random.truncated_normal(jax.random.fold_in(key, 21), -4.0, 4.0, (SEQUENCE_TOKENS, QUERY_HEADS * HEAD_SIZE), jnp.float32)
    return base_index.astype(jnp.bfloat16)


def draw_keys(key, part):
    base_index = jax.random.truncated_normal(jax.random.fold_in(key, 22), -4.0, 4.0, (SEQUENCE_TOKENS, KEY_VALUE_HEADS * HEAD_SIZE), jnp.float32)
    return base_index.astype(jnp.bfloat16)


def draw_doc_ids(key, part):
    first_len = jax.random.randint(jax.random.fold_in(key, 41), (1,), SEQUENCE_TOKENS * 5 // 8, SEQUENCE_TOKENS * 3 // 4, dtype=jnp.int32)
    others = jax.random.randint(jax.random.fold_in(key, 42), (DOCS - 2,), 0, SEQUENCE_TOKENS, dtype=jnp.int32)
    others = first_len + 1 + others % (SEQUENCE_TOKENS - first_len - 1)
    bounds = jnp.concatenate([first_len, others]).astype(jnp.int32)
    positions = jnp.arange(SEQUENCE_TOKENS, dtype=jnp.int32)
    return jnp.sum((positions[:, None] >= bounds[None, :]).astype(jnp.int32), axis=1).astype(jnp.int32)


def draw_block_lists(key, part):
    seq_devices = BLOCK_TOTAL // BPD
    remote = min(TOPK - BPD, seq_devices - 1)
    padding = TOPK - BPD - remote
    offsets = jax.random.randint(jax.random.fold_in(key, 31), (seq_devices, seq_devices), 0, BPD, dtype=jnp.int32)
    owner_ids = jnp.arange(seq_devices, dtype=jnp.int32)

    def one_row(row):
        device = row // BPD
        shuffled = jax.random.permutation(jax.random.fold_in(jax.random.fold_in(key, 32), row), seq_devices).astype(jnp.int32)
        distance = jnp.abs(owner_ids - device)
        score = shuffled + 1 + jnp.where(distance <= 2, 4 * seq_devices, 0)
        score = score + jnp.where(owner_ids == (device + seq_devices // 2) % seq_devices, 2 * seq_devices, 0)
        score = jnp.where(owner_ids != device, score, 0)
        best, chosen = lax.top_k(score, remote)
        picked = jnp.where(best > 0, chosen * BPD + offsets[device, chosen], BLOCK_TOTAL).astype(jnp.int32)
        own_blocks = (device * BPD + jnp.arange(BPD, dtype=jnp.int32)).astype(jnp.int32)
        return jnp.concatenate([own_blocks, picked, jnp.full((padding,), BLOCK_TOTAL, jnp.int32)])
    return jax.vmap(one_row)(jnp.arange(BLOCK_TOTAL, dtype=jnp.int32))


def block_scale(key, shape, cuts, smallest, high):
    factor_of, own = 1.0, jax.random.fold_in(key, 6)
    for position, parts in cuts:
        heights = jnp.exp(jax.random.uniform(jax.random.fold_in(own, position), (parts,), jnp.float32, smallest / len(cuts), high / len(cuts)))
        factor_of = factor_of * jnp.repeat(heights, shape[position] // parts).reshape([-1 if axis == position else 1 for axis in range(len(shape))])
    return factor_of


def bell_draw(own_key, extent, scale, reach, shards=(), kind=jnp.bfloat16):
    array = scale * jax.random.normal(own_key, extent, jnp.float32)
    if shards:
        array = array * block_scale(own_key, extent, shards, -0.22, 0.18)
    return jnp.clip(array, -reach, reach).astype(kind)


def setup_inputs(seed: int = 0, part: int = 0) -> dict:
    splits = jax.random.split(jax.random.key(seed), 7)
    part_splits = jax.random.split(jax.random.fold_in(splits[6], part), 7)
    queries = draw_queries(jax.random.fold_in(jax.random.fold_in(splits[6], part), 71), part)
    keys = draw_keys(jax.random.fold_in(jax.random.fold_in(splits[6], part), 71), part)
    values = bell_draw(part_splits[2], (SEQUENCE_TOKENS, KEY_VALUE_HEADS * HEAD_SIZE), 3.0, 15.0, ((0, 8), (1, 2)))
    doc_ids = draw_doc_ids(jax.random.fold_in(jax.random.fold_in(splits[6], part), 71), part)
    block_lists = draw_block_lists(jax.random.fold_in(jax.random.fold_in(splits[6], part), 71), part)
    w_out = bell_draw(splits[5], (QUERY_HEADS * HEAD_SIZE, D), (QUERY_HEADS * HEAD_SIZE) ** -0.5, 0.09375, ((0, 2),))
    return {"queries": queries, "keys": keys, "values": values, "doc_ids": doc_ids, "block_lists": block_lists, "w_out": w_out}


negative = -1e+30
far_position = 1073741824

def block_terms(query_block, key_rows, value_rows, allowed):
    scores = jnp.einsum('qhge,jkhe->hgqjk', query_block.astype(jnp.float32), key_rows.astype(jnp.float32)) * (1.0 / math.sqrt(HEAD_SIZE))
    masked = jnp.where(allowed[None, None], scores, negative)
    block_top = lax.optimization_barrier(jnp.max(masked, axis=-1))
    probs = jnp.where(allowed[None, None], jnp.exp(masked - block_top[..., None]), 0.0)
    block_sum = lax.optimization_barrier(jnp.sum(probs, axis=-1))
    weights = probs.astype(jnp.bfloat16)
    partial_value = jnp.einsum('hgqjk,jkhe->hgqje', weights.astype(jnp.float32), value_rows.astype(jnp.float32))
    return (block_top, block_sum, partial_value)

def finish(block_top, block_sum, partial_value):
    row_peak = lax.optimization_barrier(jnp.max(block_top, axis=-1))
    factor = jnp.exp(block_top - row_peak[..., None])
    numer = lax.optimization_barrier(jnp.sum(factor[..., None] * partial_value, axis=3))
    denom = lax.optimization_barrier(jnp.sum(factor * block_sum, axis=-1))
    result = numer / denom[..., None]
    rows = result.shape[2]
    return jnp.transpose(result, (2, 0, 1, 3)).reshape(rows, -1).astype(jnp.bfloat16)

def reference(queries, keys, values, doc_ids, block_lists, w_out):
    group_count = QUERY_HEADS // KEY_VALUE_HEADS
    positions = jnp.arange(SEQUENCE_TOKENS, dtype=jnp.int32)
    doc_range = jnp.arange(DOCS, dtype=jnp.int32)
    doc_match = doc_ids[:, None] == doc_range[None, :]
    firsts = lax.optimization_barrier(jnp.min(jnp.where(doc_match, positions[:, None], far_position), axis=0)).astype(jnp.int32)
    later = doc_range[None, :] > doc_range[:, None]
    ends_doc = lax.optimization_barrier(jnp.min(jnp.where(later, firsts[None, :], far_position), axis=1)).astype(jnp.int32)
    starts = lax.optimization_barrier(jnp.sum(jnp.where(doc_match, firsts[None, :], 0), axis=1)).astype(jnp.int32)
    ends = lax.optimization_barrier(jnp.sum(jnp.where(doc_match, ends_doc[None, :], 0), axis=1)).astype(jnp.int32)
    empty_block = jnp.zeros((1, BLOCK_TOKENS, KEY_VALUE_HEADS, HEAD_SIZE), jnp.bfloat16)
    key_lookup = jnp.concatenate([keys.reshape(BLOCK_TOTAL, BLOCK_TOKENS, KEY_VALUE_HEADS, HEAD_SIZE), empty_block], axis=0)
    value_lookup = jnp.concatenate([values.reshape(BLOCK_TOTAL, BLOCK_TOKENS, KEY_VALUE_HEADS, HEAD_SIZE), empty_block], axis=0)
    query_tiles = queries.reshape(BLOCK_TOTAL, BLOCK_TOKENS, KEY_VALUE_HEADS, group_count, HEAD_SIZE)
    inside = jnp.arange(BLOCK_TOKENS, dtype=jnp.int32)

    def per_block(inputs):
        query_block, lists_row, query_start, query_end = inputs
        key_rows = jnp.take(key_lookup, lists_row, axis=0)
        value_rows = jnp.take(value_lookup, lists_row, axis=0)
        usable = lists_row < BLOCK_TOTAL
        key_pos = lists_row[:, None] * BLOCK_TOKENS + inside[None, :]
        allowed = usable[None, :, None] & (key_pos[None] < query_end[:, None, None]) & (key_pos[None] >= query_start[:, None, None])
        return finish(*block_terms(query_block, key_rows, value_rows, allowed))
    attn = lax.map(per_block, (query_tiles, block_lists, starts.reshape(BLOCK_TOTAL, BLOCK_TOKENS), ends.reshape(BLOCK_TOTAL, BLOCK_TOKENS)))
    attn = attn.reshape(SEQUENCE_TOKENS, QUERY_HEADS * HEAD_SIZE)
    cols = QUERY_HEADS * HEAD_SIZE // N_HEAD

    def add_group(running, group):
        attn_cols = lax.dynamic_slice_in_dim(attn, group * cols, cols, 1)
        weight_rows = lax.dynamic_slice_in_dim(w_out, group * cols, cols, 0)
        part = jnp.dot(attn_cols, weight_rows, preferred_element_type=jnp.float32).astype(jnp.bfloat16)
        part = lax.optimization_barrier(part)
        return (running + part.astype(jnp.float32), None)
    summed, _ = lax.scan(add_group, jnp.zeros((SEQUENCE_TOKENS, D), jnp.float32), jnp.arange(N_HEAD, dtype=jnp.int32))
    return summed.astype(jnp.bfloat16)
```

```python
import functools
import math

import jax
import jax.numpy as jnp
from jax import lax
from jax.experimental import pallas as pl
from jax.experimental.pallas import tpu as pltpu
from jax.sharding import PartitionSpec as P

QUERY_HEADS = 32
KEY_VALUE_HEADS = 8
HEAD_SIZE = 128
BLOCK_TOKENS = 128
DOCS = 8
GROUP = QUERY_HEADS // KEY_VALUE_HEADS
CHUNK = 4
HALVES = 2

negative = -1e30
far_position = 1073741824
exp2_scale = math.log2(math.e) / math.sqrt(HEAD_SIZE)


def attention_kernel(
    seq_count,
    blocks_dev,
    first_block,
    own_ref,
    lists_ref,
    firsts_ref,
    docs_smem,
    docs_ref,
    q_ref,
    k_ref,
    v_ref,
    rk_ref,
    rv_ref,
    out_ref,
    ktab,
    vtab,
    scores,
    acc,
    entry,
    entry_pos,
    entry_part,
    chunk_part,
    counts,
    doc_end,
    start_row,
    end_row,
):
    h = pl.program_id(0)
    i = pl.program_id(1)
    row = first_block + i
    topk = lists_ref.shape[1]
    block_count = blocks_dev * seq_count
    slots = entry.shape[1]

    @pl.when((h == 0) & (i == 0))
    def _():
        running = jnp.int32(far_position)
        for d in range(DOCS - 1, -1, -1):
            doc_end[d] = running
            running = jnp.minimum(running, firsts_ref[d])

    @pl.when(h == 0)
    def _():
        doc_first = docs_smem[row * BLOCK_TOKENS]
        doc_last = docs_smem[row * BLOCK_TOKENS + BLOCK_TOKENS - 1]
        low, low_last = firsts_ref[doc_first], firsts_ref[doc_last]
        high_first, high = doc_end[doc_first], doc_end[doc_last]
        own = own_ref[0]
        for j in range(slots):
            entry[i, j] = jnp.int32(0)
            entry_pos[i, j] = jnp.int32(far_position)
            entry_part[i, j] = jnp.int32(1)

        def add(j, count):
            block = lists_ref[row, j]
            at = block * BLOCK_TOKENS
            used = (block < block_count) & (at < high) & (at + BLOCK_TOKENS > low)
            owner = block // blocks_dev
            whole = (at >= low_last) & (at + BLOCK_TOKENS <= high_first)

            @pl.when(used)
            def _():
                entry[i, count] = jnp.where(
                    owner == own, block - owner * blocks_dev, blocks_dev + owner
                )
                entry_pos[i, count] = at
                entry_part[i, count] = jnp.where(whole, 0, 1)

            return count + jnp.where(used, 1, 0)

        count = lax.fori_loop(0, topk, add, jnp.int32(0))
        counts[i] = (count + CHUNK - 1) // CHUNK
        for c in range(slots // CHUNK):
            part = entry_part[i, c * CHUNK]
            for s in range(1, CHUNK):
                part = part + entry_part[i, c * CHUNK + s]
            chunk_part[i, c] = part
        docs = docs_ref[0]
        start = jnp.zeros((1, BLOCK_TOKENS), jnp.int32)
        end = jnp.zeros((1, BLOCK_TOKENS), jnp.int32)
        for d in range(DOCS):
            here = docs == d
            start = jnp.where(here, firsts_ref[d], start)
            end = jnp.where(here, doc_end[d], end)
        start_row[i] = jnp.broadcast_to(start, (8, BLOCK_TOKENS))
        end_row[i] = jnp.broadcast_to(end, (8, BLOCK_TOKENS))

    @pl.when(i == 0)
    def _():
        for b in range(blocks_dev):
            ktab[b] = k_ref[pl.ds(b * BLOCK_TOKENS, BLOCK_TOKENS), :]
            vtab[b] = v_ref[pl.ds(b * BLOCK_TOKENS, BLOCK_TOKENS), :]
        ktab[pl.ds(blocks_dev, seq_count)] = rk_ref[...]
        vtab[pl.ds(blocks_dev, seq_count)] = rv_ref[...]

    width = GROUP * BLOCK_TOKENS
    keys = CHUNK * BLOCK_TOKENS
    q = jnp.concatenate(
        [q_ref[:, g * HEAD_SIZE : (g + 1) * HEAD_SIZE] for g in range(GROUP)], axis=0
    )
    chunks = counts[i]

    def fold(x, op):
        return op(x.reshape(x.shape[0] // 8, 8, width), axis=0)

    def score_step(c, top):
        at = pl.multiple_of(c * keys, keys)
        k = jnp.concatenate([ktab[entry[i, c * CHUNK + s]] for s in range(CHUNK)], axis=0)
        scores[pl.ds(at, keys), :] = lax.dot_general(
            k, q, (((1,), (1,)), ((), ())), preferred_element_type=jnp.float32
        )

        @pl.when(chunk_part[i, c] > 0)
        def _():
            start = start_row[i][0:1]
            end = end_row[i][0:1]
            start = jnp.concatenate([start] * GROUP, axis=1)
            end = jnp.concatenate([end] * GROUP, axis=1)
            inside = lax.broadcasted_iota(jnp.int32, (BLOCK_TOKENS, width), 0)
            for s in range(CHUNK):
                pos = inside + entry_pos[i, c * CHUNK + s]
                here = pl.ds(at + s * BLOCK_TOKENS, BLOCK_TOKENS)
                scores[here, :] = jnp.where(
                    (pos >= start) & (pos < end), scores[here, :], negative
                )

        return jnp.maximum(top, fold(scores[pl.ds(at, keys), :], jnp.max))

    top = lax.fori_loop(0, chunks, score_step, jnp.full((8, width), negative, jnp.float32))
    top = jnp.max(top, axis=0, keepdims=True)
    acc[...] = jnp.zeros_like(acc)

    def value_step(c, total):
        at = pl.multiple_of(c * keys, keys)
        v = jnp.concatenate([vtab[entry[i, c * CHUNK + s]] for s in range(CHUNK)], axis=0)
        p = jnp.exp2((scores[pl.ds(at, keys), :] - top) * exp2_scale)
        acc[...] += lax.dot_general(
            v,
            p.astype(jnp.bfloat16),
            (((0,), (0,)), ((), ())),
            preferred_element_type=jnp.float32,
        )
        return total + fold(p, jnp.sum)

    total = lax.fori_loop(0, chunks, value_step, jnp.zeros((8, width), jnp.float32))
    total = jnp.sum(total, axis=0, keepdims=True)
    result = acc[...] / total
    for g in range(GROUP):
        out_ref[:, g * HEAD_SIZE : (g + 1) * HEAD_SIZE] = result[
            :, g * BLOCK_TOKENS : (g + 1) * BLOCK_TOKENS
        ].T.astype(jnp.bfloat16)


def attention(half, own, lists, firsts, doc_ids, queries, keys, values, arrived):
    tok_rows = queries.shape[0]
    blocks_dev = tok_rows // BLOCK_TOKENS
    kv_heads = keys.shape[1] // HEAD_SIZE
    seq_count = arrived.shape[0]
    topk = lists.shape[1]
    slots = -(-topk // CHUNK) * CHUNK
    rows = blocks_dev // HALVES
    first_block = half * rows
    width = GROUP * BLOCK_TOKENS
    smem = pl.BlockSpec(memory_space=pltpu.SMEM)
    flops = rows * kv_heads * width * 11 * BLOCK_TOKENS * HEAD_SIZE * 4
    return pl.pallas_call(
        functools.partial(attention_kernel, seq_count, blocks_dev, first_block),
        grid=(kv_heads, rows),
        out_shape=jax.ShapeDtypeStruct((rows * BLOCK_TOKENS, queries.shape[1]), jnp.bfloat16),
        in_specs=[
            smem,
            smem,
            smem,
            smem,
            pl.BlockSpec((1, 1, BLOCK_TOKENS), lambda h, i: (first_block + i, 0, 0)),
            pl.BlockSpec((BLOCK_TOKENS, width), lambda h, i: (first_block + i, h)),
            pl.BlockSpec((tok_rows, HEAD_SIZE), lambda h, i: (0, h)),
            pl.BlockSpec((tok_rows, HEAD_SIZE), lambda h, i: (0, h)),
            pl.BlockSpec((seq_count, BLOCK_TOKENS, HEAD_SIZE), lambda h, i: (0, 0, h)),
            pl.BlockSpec((seq_count, BLOCK_TOKENS, HEAD_SIZE), lambda h, i: (0, 0, kv_heads + h)),
        ],
        out_specs=pl.BlockSpec((BLOCK_TOKENS, width), lambda h, i: (i, h)),
        scratch_shapes=[
            pltpu.VMEM((blocks_dev + seq_count, BLOCK_TOKENS, HEAD_SIZE), jnp.bfloat16),
            pltpu.VMEM((blocks_dev + seq_count, BLOCK_TOKENS, HEAD_SIZE), jnp.bfloat16),
            pltpu.VMEM((slots * BLOCK_TOKENS, width), jnp.float32),
            pltpu.VMEM((HEAD_SIZE, width), jnp.float32),
            pltpu.SMEM((rows, slots), jnp.int32),
            pltpu.SMEM((rows, slots), jnp.int32),
            pltpu.SMEM((rows, slots), jnp.int32),
            pltpu.SMEM((rows, slots // CHUNK), jnp.int32),
            pltpu.SMEM((rows,), jnp.int32),
            pltpu.SMEM((DOCS,), jnp.int32),
            pltpu.VMEM((rows, 8, BLOCK_TOKENS), jnp.int32),
            pltpu.VMEM((rows, 8, BLOCK_TOKENS), jnp.int32),
        ],
        compiler_params=pltpu.CompilerParams(
            dimension_semantics=("arbitrary", "arbitrary"), vmem_limit_bytes=40 * 2**20
        ),
        cost_estimate=pl.CostEstimate(
            flops=3 * flops, bytes_accessed=8 * 2**20, transcendentals=0
        ),
    )(
        own.reshape(1),
        lists,
        firsts,
        doc_ids,
        doc_ids.reshape(blocks_dev, 1, BLOCK_TOKENS),
        queries,
        keys,
        values,
        arrived,
        arrived,
    )


def per_device(queries, keys, values, doc_ids, block_lists, w_out):
    tok_rows = queries.shape[0]
    blocks_dev = tok_rows // BLOCK_TOKENS
    key_width = keys.shape[1]
    seq_count = lax.axis_size("seq")
    head_count = lax.axis_size("head")
    own = lax.axis_index("seq")
    head = lax.axis_index("head")
    block_count = blocks_dev * seq_count
    positions = own * tok_rows + jnp.arange(tok_rows, dtype=jnp.int32)
    doc_match = doc_ids[:, None] == jnp.arange(DOCS, dtype=jnp.int32)[None, :]
    first_local = jnp.min(jnp.where(doc_match, positions[:, None], far_position), axis=0)

    owners = jnp.arange(seq_count, dtype=jnp.int32)
    wanted = (block_lists[..., None] // blocks_dev == owners) & (
        block_lists[..., None] < block_count
    )
    request = jnp.max(
        jnp.where(wanted, block_lists[..., None] % blocks_dev + 1, 0), axis=(0, 1)
    )
    notes = lax.all_gather(jnp.concatenate([first_local, request]), "seq")
    firsts = jnp.min(notes[:, :DOCS], axis=0)
    asked = lax.dynamic_index_in_dim(notes[:, DOCS:], own, 1, keepdims=False)
    kv_blocks = jnp.concatenate([keys, values], axis=1).reshape(
        blocks_dev, BLOCK_TOKENS, 2 * key_width
    )
    outgoing = kv_blocks[jnp.maximum(asked - 1, 0)]
    arrived = lax.all_to_all(outgoing, "seq", split_axis=0, concat_axis=0, tiled=True)

    cols = w_out.shape[1] // head_count
    results = []
    for half in range(HALVES):
        attn = attention(
            half, own, block_lists, firsts, doc_ids, queries, keys, values, arrived
        )
        projected = jnp.dot(attn, w_out, preferred_element_type=jnp.float32).astype(jnp.bfloat16)
        total = lax.dynamic_slice_in_dim(projected, head * cols, cols, 1).astype(jnp.float32)
        for step in range(1, head_count):
            to = lax.rem(head + step, head_count)
            part = lax.dynamic_slice_in_dim(projected, to * cols, cols, 1)
            got = lax.ppermute(
                part, "head", [(a, (a + step) % head_count) for a in range(head_count)]
            )
            total = total + got.astype(jnp.float32)
        results.append(total.astype(jnp.bfloat16))
    return jnp.concatenate(results, axis=0)


def solution(mesh):
    in_specs = (
        P(("dp", "seq"), "head"),
        P(("dp", "seq"), "head"),
        P(("dp", "seq"), "head"),
        P(("dp", "seq")),
        P(("dp", "seq"), None),
        P("head", None),
    )
    out_specs = P(("dp", "seq"), "head")
    return jax.shard_map(
        per_device, mesh=mesh, in_specs=in_specs, out_specs=out_specs, check_vma=False
    )
```

```python
import functools
import math

import jax
import jax.numpy as jnp
from jax import lax
from jax.experimental import pallas as pl
from jax.experimental.pallas import tpu as pltpu
from jax.sharding import PartitionSpec as P

QUERY_HEADS = 32
KEY_VALUE_HEADS = 8
HEAD_SIZE = 128
BLOCK_TOKENS = 128
DOCS = 8
GROUP = QUERY_HEADS // KEY_VALUE_HEADS
CHUNK = 4
HALVES = 2
PARTS = 2
TILE = 512

negative = -1e30
far_position = 1073741824
exp2_scale = math.log2(math.e) / math.sqrt(HEAD_SIZE)


def attention_kernel(
    seq_count,
    blocks_dev,
    first_block,
    own_ref,
    lists_ref,
    notes_ref,
    docs_smem,
    docs_ref,
    q_ref,
    k_ref,
    v_ref,
    *refs,
):
    far_refs = refs[: 2 * (seq_count - 1)]
    (
    out_ref,
    ktab,
    vtab,
    scores,
    acc,
    entry,
    entry_pos,
    entry_part,
    chunk_part,
    counts,
    firsts_ref,
    doc_end,
    start_row,
    end_row,
    ) = refs[2 * (seq_count - 1) :]
    h = pl.program_id(0)
    i = pl.program_id(1)
    row = first_block + i
    topk = lists_ref.shape[1]
    block_count = blocks_dev * seq_count
    slots = entry.shape[1]

    @pl.when((h == 0) & (i == 0))
    def _():
        running = jnp.int32(far_position)
        for d in range(DOCS - 1, -1, -1):
            firsts_ref[d] = lax.fori_loop(
                0,
                seq_count,
                lambda r, low: jnp.minimum(low, notes_ref[r, d]),
                jnp.int32(far_position),
            )
            doc_end[d] = running
            running = jnp.minimum(running, firsts_ref[d])

    @pl.when(h == 0)
    def _():
        doc_first = docs_smem[row * BLOCK_TOKENS]
        doc_last = docs_smem[row * BLOCK_TOKENS + BLOCK_TOKENS - 1]
        low, low_last = firsts_ref[doc_first], firsts_ref[doc_last]
        high_first, high = doc_end[doc_first], doc_end[doc_last]
        own = own_ref[0]
        for j in range(slots):
            entry[i, j] = jnp.int32(0)
            entry_pos[i, j] = jnp.int32(far_position)
            entry_part[i, j] = jnp.int32(1)

        def add(j, count):
            block = lists_ref[row, j]
            at = block * BLOCK_TOKENS
            used = (block < block_count) & (at < high) & (at + BLOCK_TOKENS > low)
            owner = block // blocks_dev
            whole = (at >= low_last) & (at + BLOCK_TOKENS <= high_first)

            @pl.when(used)
            def _():
                entry[i, count] = jnp.where(
                    owner == own,
                    block - owner * blocks_dev,
                    blocks_dev - 1 + lax.rem(own - owner + seq_count, seq_count),
                )
                entry_pos[i, count] = at
                entry_part[i, count] = jnp.where(whole, 0, 1)

            return count + jnp.where(used, 1, 0)

        count = lax.fori_loop(0, topk, add, jnp.int32(0))
        counts[i] = (count + CHUNK - 1) // CHUNK
        for c in range(slots // CHUNK):
            part = entry_part[i, c * CHUNK]
            for s in range(1, CHUNK):
                part = part + entry_part[i, c * CHUNK + s]
            chunk_part[i, c] = part
        docs = docs_ref[0]
        start = jnp.zeros((1, BLOCK_TOKENS), jnp.int32)
        end = jnp.zeros((1, BLOCK_TOKENS), jnp.int32)
        for d in range(DOCS):
            here = docs == d
            start = jnp.where(here, firsts_ref[d], start)
            end = jnp.where(here, doc_end[d], end)
        start_row[i] = jnp.broadcast_to(start, (8, BLOCK_TOKENS))
        end_row[i] = jnp.broadcast_to(end, (8, BLOCK_TOKENS))

    @pl.when(i == 0)
    def _():
        for b in range(blocks_dev):
            ktab[b] = k_ref[pl.ds(b * BLOCK_TOKENS, BLOCK_TOKENS), :]
            vtab[b] = v_ref[pl.ds(b * BLOCK_TOKENS, BLOCK_TOKENS), :]
        for d in range(seq_count - 1):
            ktab[blocks_dev + d] = far_refs[2 * d][...]
            vtab[blocks_dev + d] = far_refs[2 * d + 1][...]

    width = GROUP * BLOCK_TOKENS
    keys = CHUNK * BLOCK_TOKENS
    q = jnp.concatenate(
        [q_ref[:, g * HEAD_SIZE : (g + 1) * HEAD_SIZE] for g in range(GROUP)], axis=0
    )
    chunks = counts[i]

    def fold(x, op):
        return op(x.reshape(x.shape[0] // 8, 8, width), axis=0)

    def score_step(c, top):
        at = pl.multiple_of(c * keys, keys)
        k = jnp.concatenate([ktab[entry[i, c * CHUNK + s]] for s in range(CHUNK)], axis=0)
        scores[pl.ds(at, keys), :] = lax.dot_general(
            k, q, (((1,), (1,)), ((), ())), preferred_element_type=jnp.float32
        )

        @pl.when(chunk_part[i, c] > 0)
        def _():
            start = start_row[i][0:1]
            end = end_row[i][0:1]
            start = jnp.concatenate([start] * GROUP, axis=1)
            end = jnp.concatenate([end] * GROUP, axis=1)
            inside = lax.broadcasted_iota(jnp.int32, (BLOCK_TOKENS, width), 0)
            for s in range(CHUNK):
                pos = inside + entry_pos[i, c * CHUNK + s]
                here = pl.ds(at + s * BLOCK_TOKENS, BLOCK_TOKENS)
                scores[here, :] = jnp.where(
                    (pos >= start) & (pos < end), scores[here, :], negative
                )

        return jnp.maximum(top, fold(scores[pl.ds(at, keys), :], jnp.max))

    top = lax.fori_loop(0, chunks, score_step, jnp.full((8, width), negative, jnp.float32))
    top = jnp.max(top, axis=0, keepdims=True)
    acc[...] = jnp.zeros_like(acc)

    def value_step(c, total):
        at = pl.multiple_of(c * keys, keys)
        v = jnp.concatenate([vtab[entry[i, c * CHUNK + s]] for s in range(CHUNK)], axis=0)
        p = jnp.exp2((scores[pl.ds(at, keys), :] - top) * exp2_scale)
        acc[...] += lax.dot_general(
            v,
            p.astype(jnp.bfloat16),
            (((0,), (0,)), ((), ())),
            preferred_element_type=jnp.float32,
        )
        return total + fold(p, jnp.sum)

    total = lax.fori_loop(0, chunks, value_step, jnp.zeros((8, width), jnp.float32))
    total = jnp.sum(total, axis=0, keepdims=True)
    result = acc[...] / total
    for g in range(GROUP):
        out_ref[:, g * HEAD_SIZE : (g + 1) * HEAD_SIZE] = result[
            :, g * BLOCK_TOKENS : (g + 1) * BLOCK_TOKENS
        ].T.astype(jnp.bfloat16)


def attention(half, part, own, lists, notes, doc_ids, queries, keys, values, arrived):
    tok_rows = queries.shape[0]
    blocks_dev = tok_rows // BLOCK_TOKENS
    kv_heads = arrived[0].shape[1] // (2 * HEAD_SIZE)
    first_head = part * kv_heads
    seq_count = len(arrived) + 1
    topk = lists.shape[1]
    slots = -(-topk // CHUNK) * CHUNK
    rows = blocks_dev // HALVES
    first_block = half * rows
    width = GROUP * BLOCK_TOKENS
    smem = pl.BlockSpec(memory_space=pltpu.SMEM)
    flops = rows * kv_heads * width * 11 * BLOCK_TOKENS * HEAD_SIZE * 4
    return pl.pallas_call(
        functools.partial(attention_kernel, seq_count, blocks_dev, first_block),
        grid=(kv_heads, rows),
        out_shape=jax.ShapeDtypeStruct((rows * BLOCK_TOKENS, kv_heads * width), jnp.bfloat16),
        in_specs=[
            smem,
            smem,
            smem,
            smem,
            pl.BlockSpec((1, 1, BLOCK_TOKENS), lambda h, i: (first_block + i, 0, 0)),
            pl.BlockSpec((BLOCK_TOKENS, width), lambda h, i: (first_block + i, first_head + h)),
            pl.BlockSpec((tok_rows, HEAD_SIZE), lambda h, i: (0, first_head + h)),
            pl.BlockSpec((tok_rows, HEAD_SIZE), lambda h, i: (0, first_head + h)),
        ]
        + [
            pl.BlockSpec((BLOCK_TOKENS, HEAD_SIZE), lambda h, i: (0, h)),
            pl.BlockSpec((BLOCK_TOKENS, HEAD_SIZE), lambda h, i: (0, kv_heads + h)),
        ]
        * len(arrived),
        out_specs=pl.BlockSpec((BLOCK_TOKENS, width), lambda h, i: (i, h)),
        scratch_shapes=[
            pltpu.VMEM((blocks_dev + seq_count - 1, BLOCK_TOKENS, HEAD_SIZE), jnp.bfloat16),
            pltpu.VMEM((blocks_dev + seq_count - 1, BLOCK_TOKENS, HEAD_SIZE), jnp.bfloat16),
            pltpu.VMEM((slots * BLOCK_TOKENS, width), jnp.float32),
            pltpu.VMEM((HEAD_SIZE, width), jnp.float32),
            pltpu.SMEM((rows, slots), jnp.int32),
            pltpu.SMEM((rows, slots), jnp.int32),
            pltpu.SMEM((rows, slots), jnp.int32),
            pltpu.SMEM((rows, slots // CHUNK), jnp.int32),
            pltpu.SMEM((rows,), jnp.int32),
            pltpu.SMEM((DOCS,), jnp.int32),
            pltpu.SMEM((DOCS,), jnp.int32),
            pltpu.VMEM((rows, 8, BLOCK_TOKENS), jnp.int32),
            pltpu.VMEM((rows, 8, BLOCK_TOKENS), jnp.int32),
        ],
        compiler_params=pltpu.CompilerParams(
            dimension_semantics=("arbitrary", "arbitrary"), vmem_limit_bytes=24 * 2**20
        ),
        cost_estimate=pl.CostEstimate(
            flops=3 * flops, bytes_accessed=8 * 2**20, transcendentals=0
        ),
    )(
        own.reshape(1),
        lists,
        notes,
        doc_ids,
        doc_ids.reshape(blocks_dev, 1, BLOCK_TOKENS),
        queries,
        keys,
        values,
        *[x for pair in zip(arrived, arrived) for x in pair],
    )


def pick_kernel(parts, seq_count, own_ref, notes_ref, k_ref, v_ref, *out_refs):
    width = k_ref.shape[1] // parts
    own = own_ref[0]
    for d in range(1, seq_count):
        asked = notes_ref[lax.rem(own + d, seq_count), DOCS + own]
        at = jnp.maximum(asked - 1, 0) * BLOCK_TOKENS
        rows = pl.ds(pl.multiple_of(at, BLOCK_TOKENS), BLOCK_TOKENS)
        for part in range(parts):
            cols = slice(part * width, (part + 1) * width)
            out_ref = out_refs[part * (seq_count - 1) + d - 1]
            out_ref[:, :width] = k_ref[rows, cols]
            out_ref[:, width:] = v_ref[rows, cols]


def pick(parts, own, notes, keys, values):
    seq_count = notes.shape[0]
    width = keys.shape[1] // parts
    smem = pl.BlockSpec(memory_space=pltpu.SMEM)
    vmem = pl.BlockSpec(memory_space=pltpu.VMEM)
    count = parts * (seq_count - 1)
    flat = pl.pallas_call(
        functools.partial(pick_kernel, parts, seq_count),
        out_shape=[jax.ShapeDtypeStruct((BLOCK_TOKENS, 2 * width), jnp.bfloat16)] * count,
        in_specs=[smem, smem, vmem, vmem],
        out_specs=[vmem] * count,
        cost_estimate=pl.CostEstimate(flops=0, bytes_accessed=4 * 2**20, transcendentals=0),
        compiler_params=pltpu.CompilerParams(vmem_limit_bytes=24 * 2**20),
    )(own.reshape(1), notes, keys, values)
    return [flat[p * (seq_count - 1) : (p + 1) * (seq_count - 1)] for p in range(parts)]


def project_kernel(groups, at_ref, *refs):
    w_ref, out_ref, held = refs[-3:]
    attn_refs = refs[:-3]

    @pl.when((pl.program_id(0) == 0) & (pl.program_id(1) == 0))
    def _():
        row = 0
        for group in groups:
            col = 0
            for ref in attn_refs[group[0] : group[1]]:
                held[row : row + ref.shape[0], col : col + ref.shape[1]] = ref[...]
                col += ref.shape[1]
            row += attn_refs[group[0]].shape[0]

    out_ref[0] = jnp.dot(
        held[...], w_ref[...], preferred_element_type=jnp.float32
    ).astype(jnp.bfloat16)


def project(halves, starts, w_out, cols):
    count = starts.shape[0]
    tile = min(TILE, cols)
    tiles = cols // tile
    depth = w_out.shape[0]
    rows = sum(half[0].shape[0] for half in halves)
    groups, operands = [], []
    for half in halves:
        groups.append((len(operands), len(operands) + len(half)))
        operands += half
    return pl.pallas_call(
        functools.partial(project_kernel, tuple(groups)),
        grid_spec=pltpu.PrefetchScalarGridSpec(
            num_scalar_prefetch=1,
            grid=(count, tiles),
            in_specs=[pl.BlockSpec(a.shape, lambda s, t, at: (0, 0)) for a in operands]
            + [pl.BlockSpec((depth, tile), lambda s, t, at: (0, at[s] * tiles + t))],
            out_specs=pl.BlockSpec((1, rows, tile), lambda s, t, at: (s, 0, t)),
            scratch_shapes=[pltpu.VMEM((rows, depth), jnp.bfloat16)],
        ),
        out_shape=jax.ShapeDtypeStruct((count, rows, cols), jnp.bfloat16),
        cost_estimate=pl.CostEstimate(
            flops=2 * rows * depth * cols * count,
            bytes_accessed=2 * depth * cols * count,
            transcendentals=0,
        ),
        compiler_params=pltpu.CompilerParams(
            dimension_semantics=("arbitrary", "arbitrary"), vmem_limit_bytes=24 * 2**20
        ),
    )(starts, *operands, w_out)


def add_kernel(own_ref, *refs):
    out_ref = refs[-1]
    total = own_ref[0].astype(jnp.float32)
    for ref in refs[:-1]:
        if len(ref.shape) == 2 and ref.shape == out_ref.shape:
            total = total + ref[...].astype(jnp.float32)
    out_ref[...] = total.astype(jnp.bfloat16)


def add_rows(half, own, got, filled):
    rows, cols = got[0].shape
    step = min(64, rows)
    first = half * rows // step
    specs = [pl.BlockSpec((1, step, cols), lambda r: (0, first + r, 0))]
    specs += [pl.BlockSpec((step, cols), lambda r: (r, 0))] * len(got)
    operands = [own] + got
    aliases = {}
    if filled is not None:
        aliases = {len(operands): 0}
        specs.append(pl.BlockSpec(memory_space=pl.ANY))
        operands.append(filled)
    return pl.pallas_call(
        add_kernel,
        grid=(rows // step,),
        out_shape=jax.ShapeDtypeStruct(own.shape[1:], jnp.bfloat16),
        in_specs=specs,
        out_specs=pl.BlockSpec((step, cols), lambda r: (first + r, 0)),
        input_output_aliases=aliases,
        cost_estimate=pl.CostEstimate(
            flops=rows * cols, bytes_accessed=6 * rows * cols, transcendentals=0
        ),
        compiler_params=pltpu.CompilerParams(vmem_limit_bytes=16 * 2**20),
    )(*operands)


def per_device(queries, keys, values, doc_ids, block_lists, w_out):
    tok_rows = queries.shape[0]
    blocks_dev = tok_rows // BLOCK_TOKENS
    key_width = keys.shape[1]
    seq_count = lax.axis_size("seq")
    head_count = lax.axis_size("head")
    own = lax.axis_index("seq")
    head = lax.axis_index("head")
    block_count = blocks_dev * seq_count
    positions = own * tok_rows + jnp.arange(tok_rows, dtype=jnp.int32)
    doc_match = doc_ids[:, None] == jnp.arange(DOCS, dtype=jnp.int32)[None, :]
    first_local = jnp.min(jnp.where(doc_match, positions[:, None], far_position), axis=0)

    owners = jnp.arange(seq_count, dtype=jnp.int32)
    wanted = (block_lists[..., None] // blocks_dev == owners) & (
        block_lists[..., None] < block_count
    )
    request = jnp.max(
        jnp.where(wanted, block_lists[..., None] % blocks_dev + 1, 0), axis=(0, 1)
    )
    notes = lax.all_gather(jnp.concatenate([first_local, request]), "seq")
    kv_heads = key_width // HEAD_SIZE
    parts = math.gcd(kv_heads, PARTS)
    outgoing = pick(parts, own, notes, keys, values)
    attn = [[] for _ in range(HALVES)]
    arrived = [
        [
            lax.ppermute(x, "seq", [(a, (a + d) % seq_count) for a in range(seq_count)])
            for d, x in enumerate(sent, 1)
        ]
        for sent in outgoing
    ]
    for part in range(parts):
        for half in range(HALVES):
            attn[half].append(
                attention(
                    half, part, own, block_lists, notes, doc_ids, queries, keys, values,
                    arrived[part],
                )
            )

    cols = w_out.shape[1] // head_count
    others = lax.rem(head + jnp.arange(1, head_count, dtype=jnp.int32), head_count)
    got = []
    for half in range(HALVES):
        shares = project([attn[half]], others, w_out, cols)
        got.append(
            [
                lax.ppermute(
                    shares[step - 1],
                    "head",
                    [(a, (a + step) % head_count) for a in range(head_count)],
                )
                for step in range(1, head_count)
            ]
        )
    kept = project(attn, head.reshape(1), w_out, cols)
    out = None
    for half in range(HALVES):
        out = add_rows(half, kept, got[half], out)
    return out


def solution(mesh):
    in_specs = (
        P(("dp", "seq"), "head"),
        P(("dp", "seq"), "head"),
        P(("dp", "seq"), "head"),
        P(("dp", "seq")),
        P(("dp", "seq"), None),
        P("head", None),
    )
    out_specs = P(("dp", "seq"), "head")
    return jax.shard_map(
        per_device, mesh=mesh, in_specs=in_specs, out_specs=out_specs, check_vma=False
    )
```
